32 devices in a mesh: rows: 8 (over z, y), rep: 4 (over x, core).
Axes of the slice: x: 2, y: 2, z: 4, core: 2. Of those that a mesh axis runs over, the one named last changes fastest.
Arguments:
- embeddings: bfloat16 [2048, 1024], P('rows', 'rep'), may hold values from -6 to 6
- coarse_ids: int32 [2048], P('rows'), may hold values from 0 to 255
- fine_ids: int32 [2048], P('rows'), may hold values from 0 to 65535, as said below
- pq_codes: int32 [2048, 64], P('rows', 'rep'), may hold values from 0 to 255
- old_coarse: float32 [256, 1024], P(None, 'rep'), may hold values from -3 to 3
- old_fine: float32 [65536, 1024], P('rows', 'rep'), may hold values from -3 to 3
- old_codebook: float32 [256, 1024], P('rows', 'rep'), may hold values from -3 to 3
Outputs:
- new_coarse: float32 [256, 1024], P(None, 'rep')
- new_fine: float32 [65536, 1024], P('rows', 'rep')
- residual: bfloat16 [2048, 1024], P('rows', 'rep')
- new_codebook: float32 [256, 1024], P('rows', 'rep')
- row_error: float32 [2048], P('rows')
The draws below stay inside these ranges and needn't reach their ends.
Inputs may be any that keep to these rules, and one draw needn't show every extreme that they name: `fine_ids`: within each aligned block of 256 rows, at most 128 ids lie in any one range o * 8192 to (o + 1) * 8192 - 1, and in every block some range holds exactly 128 of them.
All inputs are finite; a program needn't handle non-finite values.
Results may differ from the reference program's by a relative error of at most 0.0049.
Values may be sent and summed in bfloat16 or wider, within the bound.
No kernel may reach another device: no remote copies, remote signals or barrier semaphores. Data moves between devices by JAX's collectives and lax.ppermute only.
A program may use at most 64 MiB of HBM per device.

```python
import math
import jax
import jax.numpy as jnp
import numpy as np
from jax import lax

D = 1024
NCOARSE = 256
NFINE = 65536
M = 64
KSUB = 256
ROW_DEV = 256
DSUB = 16
NROWS = 2048
FINE_DEV = 8192
CAP = 128
N_ROWS = 8


def draw_fine_ids(key, part):
    base = jax.random.fold_in(key, 11)
    random_keys = jax.random.split(base, 7)
    owner_rows = N_ROWS
    candidate_count = owner_rows * CAP
    heavy_total = max(1, owner_rows // 16)
    order = jax.random.permutation(random_keys[0], owner_rows)
    heavy_clusters = jnp.zeros((owner_rows,), jnp.int32).at[order[:heavy_total]].set(1)
    noise_extra = jax.random.randint(random_keys[1], (N_ROWS, owner_rows), 0, 2)
    extra_score = jnp.where(heavy_clusters[None, :] == 1, 3, noise_extra)
    owner_of_slot = jnp.arange(candidate_count, dtype=jnp.int32) // CAP
    random_portion = jax.random.randint(random_keys[2], (N_ROWS, candidate_count), 0, 4096)
    owner_scores = (extra_score[:, owner_of_slot] * 4096 + random_portion) * candidate_count + jnp.arange(candidate_count, dtype=jnp.int32)[None, :]
    _, chosen = lax.top_k(owner_scores, ROW_DEV)
    chosen = jax.random.permutation(random_keys[3], chosen, axis=1, independent=True)
    owner_ids = chosen // CAP
    first = jax.random.randint(random_keys[4], (N_ROWS, ROW_DEV), 0, FINE_DEV)
    second = jax.random.randint(random_keys[5], (N_ROWS, ROW_DEV), 0, FINE_DEV)
    offsets = jax.random.randint(random_keys[6], (owner_rows,), 0, FINE_DEV)
    local_ids = (first * second // FINE_DEV + offsets[owner_ids]) % FINE_DEV
    return (owner_ids * FINE_DEV + local_ids).reshape(-1).astype(jnp.int32)


def set_ends(array, key, low, high):
    place = [jax.random.randint(jax.random.fold_in(key, axis), (), 0, length) for axis, length in enumerate(array.shape)]
    main_axis = array.shape.index(max(array.shape))
    beside = place[:main_axis] + [(place[main_axis] + 1) % array.shape[main_axis]] + place[main_axis + 1:]
    return array.at[tuple(place)].set(low).at[tuple(beside)].set(high)


def steps_of(stream_key, extent, shards, smallest, largest):
    loudness, own = 1.0, jax.random.fold_in(stream_key, 6)
    for axis_at, blocks in shards:
        steps = jnp.exp(jax.random.uniform(jax.random.fold_in(own, axis_at), (blocks,), jnp.float32, smallest / len(shards), largest / len(shards)))
        loudness = loudness * jnp.repeat(steps, extent[axis_at] // blocks).reshape([-1 if axis == axis_at else 1 for axis in range(len(extent))])
    return loudness


def rank_bounds(amount, skew):
    portions = [(1 << 20) // math.isqrt(standing ** skew) + 1 for standing in range(1, amount + 1)]
    spread = 1 + sum(portions) // (1 << 30)
    return np.cumsum(np.array([max(1, weight // spread) for weight in portions]))


def skewed_ids(key, shape, number_of, lean):
    grid = rank_bounds(number_of, lean)
    lot = jax.random.randint(jax.random.fold_in(key, 1), shape, 0, int(grid[number_of - 1]))
    rank = jnp.searchsorted(jnp.asarray(grid, jnp.int32), lot, side="right")
    return jax.random.permutation(jax.random.fold_in(key, 2), number_of)[rank].astype(jnp.int32)


def scatter_about(own_key, shape, deviation, bound, cuts=(), kind=jnp.bfloat16):
    values = deviation * jax.random.normal(own_key, shape, jnp.float32)
    if cuts:
        values = values * steps_of(own_key, shape, cuts, -0.22, 0.18)
    return jnp.clip(values, -bound, bound).astype(kind)


def setup_inputs(seed: int = 0) -> dict:
    streams_of = jax.random.split(jax.random.key(seed), 8)
    embeddings = scatter_about(streams_of[0], (NROWS, D), 1.0, 6.0, ((0, 8), (1, 4)))
    coarse_ids = set_ends(skewed_ids(streams_of[1], (NROWS,), NCOARSE, 4), jax.random.fold_in(streams_of[1], 3), 0, NCOARSE - 1).astype(jnp.int32)
    fine_ids = draw_fine_ids(jax.random.fold_in(streams_of[7], 71), 0)
    pq_codes = set_ends(skewed_ids(streams_of[3], (NROWS, M), KSUB, 4), jax.random.fold_in(streams_of[3], 3), 0, KSUB - 1).astype(jnp.int32)
    old_coarse = scatter_about(streams_of[4], (NCOARSE, D), 0.5, 3.0, ((1, 4),), jnp.float32)
    old_fine = scatter_about(streams_of[5], (NFINE, D), 0.5, 3.0, ((0, 8), (1, 4)), jnp.float32)
    old_codebook = scatter_about(streams_of[6], (KSUB, D), 0.5, 3.0, ((0, 8), (1, 4)), jnp.float32)
    return dict(embeddings=embeddings, coarse_ids=coarse_ids, fine_ids=fine_ids, pq_codes=pq_codes, old_coarse=old_coarse, old_fine=old_fine, old_codebook=old_codebook)


def update_means(sums, counts, fallback):
    return jnp.where(counts[:, None] > 0, sums / jnp.maximum(counts, 1.0)[:, None], fallback)


def reference(embeddings, coarse_ids, fine_ids, pq_codes, old_coarse, old_fine, old_codebook):
    ones_rows = jnp.ones((NROWS,), jnp.float32)
    coarse_sum = jax.ops.segment_sum(embeddings.astype(jnp.float32), coarse_ids, num_segments=NCOARSE)
    coarse_count = jax.ops.segment_sum(ones_rows, coarse_ids, num_segments=NCOARSE)
    new_coarse = update_means(coarse_sum, coarse_count, old_coarse)
    coarse_residual = (embeddings.astype(jnp.float32) - new_coarse[coarse_ids]).astype(jnp.bfloat16)
    fine_sum = jax.ops.segment_sum(coarse_residual.astype(jnp.float32), fine_ids, num_segments=NFINE)
    fine_count = jax.ops.segment_sum(ones_rows, fine_ids, num_segments=NFINE)
    new_fine = update_means(fine_sum, fine_count, old_fine)
    residual = (coarse_residual.astype(jnp.float32) - new_fine[fine_ids]).astype(jnp.bfloat16)
    pieces = residual.astype(jnp.float32).reshape(NROWS, M, DSUB)
    segment_ids = (pq_codes + KSUB * jnp.arange(M, dtype=jnp.int32)[None, :]).astype(jnp.int32)
    code_sum = jax.ops.segment_sum(pieces.reshape(NROWS * M, DSUB), segment_ids.reshape(-1), num_segments=M * KSUB)
    code_sum = code_sum.reshape(M, KSUB, DSUB)
    code_count = jax.ops.segment_sum(jnp.ones((NROWS * M,), jnp.float32), segment_ids.reshape(-1), num_segments=M * KSUB)
    code_count = code_count.reshape(M, KSUB)
    old_view = old_codebook.reshape(KSUB, M, DSUB).transpose(1, 0, 2)
    book_means = jnp.where(code_count[:, :, None] > 0, code_sum / jnp.maximum(code_count, 1.0)[:, :, None], old_view)
    rebuilt = book_means[jnp.arange(M, dtype=jnp.int32)[None, :], pq_codes]
    differ = pieces - rebuilt
    row_error = jnp.sum(differ * differ, axis=(1, 2)) / D
    new_codebook = book_means.transpose(1, 0, 2).reshape(KSUB, D)
    return new_coarse, new_fine, residual, new_codebook, row_error
```

```python
import functools
import math

import jax
import jax.numpy as jnp
from jax import lax
from jax.experimental import pallas as pl
from jax.experimental.pallas import tpu as pltpu
from jax.sharding import PartitionSpec as P


def update_means(sums, counts, fallback):
    return jnp.where(counts[:, None] > 0, sums / jnp.maximum(counts, 1.0)[:, None], fallback)


def exchange_shards(embeddings, coarse_ids, fine_ids, pq_codes, old_coarse, old_fine, old_codebook):
    owner_rows = lax.axis_size("rows")
    row_total, width_dev = embeddings.shape
    coarse_total = old_coarse.shape[0]
    coarse_hot = coarse_ids[None, :] == jnp.arange(coarse_total, dtype=jnp.int32)[:, None]
    coarse_sum = jnp.dot(
        coarse_hot.astype(jnp.bfloat16), embeddings, preferred_element_type=jnp.float32
    )
    coarse_count = jnp.sum(coarse_hot, axis=1).astype(jnp.float32)
    coarse_sum, coarse_count = lax.psum((coarse_sum, coarse_count), "rows")
    new_coarse = update_means(coarse_sum, coarse_count, old_coarse)
    coarse_residual = (
        embeddings.astype(jnp.float32) - jnp.take(new_coarse, coarse_ids, axis=0)
    ).astype(jnp.bfloat16)
    fine_dev = old_fine.shape[0]
    capacity = 4 * row_total // owner_rows
    slot_total = owner_rows * capacity
    owner_ids = fine_ids // fine_dev
    local_ids = fine_ids % fine_dev
    owner_hot = (owner_ids[:, None] == jnp.arange(owner_rows, dtype=jnp.int32)[None, :]).astype(
        jnp.int32
    )
    rank_in = jnp.sum(jnp.cumsum(owner_hot, axis=0) * owner_hot, axis=1) - 1
    slot_of_row = owner_ids * capacity + rank_in
    row_of_slot = (
        jnp.full((slot_total,), row_total, jnp.int32)
        .at[slot_of_row]
        .set(jnp.arange(row_total, dtype=jnp.int32))
    )
    send_rows = jnp.take(coarse_residual, row_of_slot, axis=0, mode="fill", fill_value=0).reshape(
        owner_rows, capacity, width_dev
    )
    send_ids = (
        jnp.full((slot_total,), -1, jnp.int32)
        .at[slot_of_row]
        .set(local_ids)
        .reshape(owner_rows, capacity)
    )
    recv_rows, recv_ids = (
        lax.all_to_all(send_rows, "rows", split_axis=0, concat_axis=0, tiled=True),
        lax.all_to_all(send_ids, "rows", split_axis=0, concat_axis=0, tiled=True),
    )
    rows_flat = recv_rows.reshape(slot_total, width_dev)
    ids_flat = recv_ids.reshape(slot_total)
    block_size = math.gcd(slot_total, 2048)
    fine_range = jnp.arange(fine_dev, dtype=jnp.int32)

    def fine_step(running, pieces):
        sums, counts = running
        block_rows, block_ids = pieces
        one_hot = block_ids[None, :] == fine_range[:, None]
        sums = sums + jnp.dot(
            one_hot.astype(jnp.bfloat16), block_rows, preferred_element_type=jnp.float32
        )
        counts = counts + jnp.sum(one_hot, axis=1).astype(jnp.float32)
        return ((sums, counts), None)

    start_fine = (
        jnp.zeros((fine_dev, width_dev), jnp.float32),
        jnp.zeros((fine_dev,), jnp.float32),
    )
    (fine_sum, fine_count), _ = lax.scan(
        fine_step,
        start_fine,
        (
            rows_flat.reshape(slot_total // block_size, block_size, width_dev),
            ids_flat.reshape(slot_total // block_size, block_size),
        ),
    )
    new_fine = update_means(fine_sum, fine_count, old_fine)
    safe_ids = jnp.maximum(ids_flat, 0)
    at_owner = (rows_flat.astype(jnp.float32) - jnp.take(new_fine, safe_ids, axis=0)).astype(
        jnp.bfloat16
    )
    returned = lax.all_to_all(
        at_owner.reshape(owner_rows, capacity, width_dev),
        "rows",
        split_axis=0,
        concat_axis=0,
        tiled=True,
    ).reshape(slot_total, width_dev)
    residual = jnp.take(returned, slot_of_row, axis=0)
    sub_dev = pq_codes.shape[1]
    sub_width = width_dev // sub_dev
    share_codes = old_codebook.shape[0]
    book_rows = share_codes * owner_rows
    code_block = math.gcd(row_total, 512)
    code_range = jnp.arange(book_rows, dtype=jnp.int32)

    def code_step(running, pieces):
        sums, counts = running
        block_rows, block_codes = pieces
        one_hot = block_codes.T[:, None, :] == code_range[None, :, None]
        split_rows = block_rows.reshape(code_block, sub_dev, sub_width)
        sums = sums + jnp.einsum(
            "mkn,nmd->kmd",
            one_hot.astype(jnp.bfloat16),
            split_rows,
            preferred_element_type=jnp.float32,
        )
        counts = counts + jnp.sum(one_hot, axis=2).T.astype(jnp.float32)
        return ((sums, counts), None)

    start_code = (
        jnp.zeros((book_rows, sub_dev, sub_width), jnp.float32),
        jnp.zeros((book_rows, sub_dev), jnp.float32),
    )
    (code_sum, code_count), _ = lax.scan(
        code_step,
        start_code,
        (
            residual.reshape(row_total // code_block, code_block, width_dev),
            pq_codes.reshape(row_total // code_block, code_block, sub_dev),
        ),
    )
    code_sum = code_sum.reshape(book_rows, width_dev)
    code_sum, code_count = lax.psum((code_sum, code_count), "rows")
    column_count = jnp.repeat(code_count, sub_width, axis=1)
    averages = code_sum / jnp.maximum(column_count, 1.0)
    first_code = lax.axis_index("rows") * share_codes
    own_count = lax.dynamic_slice_in_dim(column_count, first_code, share_codes, 0)
    own_average = lax.dynamic_slice_in_dim(averages, first_code, share_codes, 0)
    new_codebook = jnp.where(own_count > 0, own_average, old_codebook)
    book_view = averages.reshape(book_rows, sub_dev, sub_width)
    rebuilt = book_view[pq_codes, jnp.arange(sub_dev, dtype=jnp.int32)[None, :]].reshape(
        row_total, width_dev
    )
    differ = residual.astype(jnp.float32) - rebuilt
    partial_error = jnp.sum(differ * differ, axis=1)
    row_error = lax.psum(partial_error, "rep") / (width_dev * lax.axis_size("rep"))
    return (new_coarse, new_fine, residual, new_codebook, row_error)


PACK = 16
NN = (((1,), (0,)), ((), ()))
NT = (((1,), (1,)), ((), ()))


def mm(left, right, dims):
    return lax.dot_general(left, right, dims, preferred_element_type=jnp.float32)


def thirds(value):
    high = value.astype(jnp.bfloat16)
    rest = value - high.astype(jnp.float32)
    middle = rest.astype(jnp.bfloat16)
    low = (rest - middle.astype(jnp.float32)).astype(jnp.bfloat16)
    return jnp.concatenate([high, middle, low], axis=0)


def whole(pieces):
    size = pieces.shape[0] // 3
    return (pieces[:size] + pieces[size : 2 * size]) + pieces[2 * size :]


def pack_kernel(emb_ref, coarse_ref, fine_ref, codes_ref, out_ref):
    width = emb_ref.shape[1]
    rows = emb_ref.shape[0]
    out_ref[:width] = emb_ref[...].T
    fine = fine_ref[...]
    place = lax.broadcasted_iota(jnp.int32, (PACK, rows), 0)
    ids = jnp.where(
        place == 0,
        1,
        jnp.where(
            place == 1, coarse_ref[...], jnp.where(place == 2, fine >> 8, jnp.where(place == 3, fine & 255, 0))
        ),
    )
    out_ref[width : width + PACK] = ids.astype(jnp.float32).astype(jnp.bfloat16)
    out_ref[width + PACK :] = codes_ref[...].astype(jnp.float32).T.astype(jnp.bfloat16)


def steps_kernel(blocks, *refs):
    parts = refs[:blocks]
    (old_coarse_ref, old_book_ref, old_fine_ref) = refs[blocks : blocks + 3]
    (new_coarse_ref, new_fine_ref, residual_ref, new_book_ref, error_ref) = refs[blocks + 3 : blocks + 8]
    (table, feat, hot, crs, mean_rows, res, books, counts, slots_v, slots_s, in_sem, out_sem, list_sem) = refs[
        blocks + 8 :
    ]
    coarse_total, width = old_coarse_ref.shape
    share = old_book_ref.shape[0]
    fine_dev = old_fine_ref.shape[0]
    rows = parts[0].shape[1]
    total = rows * blocks
    sub_dev = parts[0].shape[0] - width - PACK
    sub_width = width // sub_dev
    code_total = share * blocks
    me = lax.axis_index("rows")

    load = pltpu.make_async_copy(old_fine_ref, table, in_sem)
    load.start()
    for b in range(blocks):
        feat[:, b * rows : (b + 1) * rows] = parts[b][...]

    slot_max = slots_s.shape[1] // 2
    digits = [
        jnp.concatenate([parts[b][width + 2 + d : width + 3 + d].astype(jnp.float32) for b in range(blocks)], axis=0)
        for d in range(2)
    ]
    ids8 = (digits[0] * 256.0 + digits[1]).astype(jnp.int32)
    local8 = ids8 - me * fine_dev
    mine = jnp.logical_and(local8 >= 0, local8 < fine_dev)
    mine_f = jnp.where(mine, 1.0, 0.0)
    earlier = lax.broadcasted_iota(jnp.int32, (rows, rows), 0) < lax.broadcasted_iota(jnp.int32, (rows, rows), 1)
    rank = mm(mine_f.astype(jnp.bfloat16), jnp.where(earlier, 1.0, 0.0).astype(jnp.bfloat16), NN)
    rank = jnp.where(mine, rank.astype(jnp.int32), -1)
    local8 = jnp.where(mine, local8, 0)
    lane = lax.broadcasted_iota(jnp.int32, (1, rows), 1)
    slot_at = lax.broadcasted_iota(jnp.int32, (slot_max, rows), 0)
    for b in range(blocks):
        pick = jnp.where(slot_at == rank[b : b + 1], 1.0, 0.0).astype(jnp.bfloat16)
        mine_b = local8[b : b + 1]
        values = jnp.concatenate(
            [(mine_b >> 8).astype(jnp.float32), (mine_b & 255).astype(jnp.float32), lane.astype(jnp.float32)]
            + [jnp.zeros((5, rows), jnp.float32)],
            axis=0,
        ).astype(jnp.bfloat16)
        got = mm(values, pick, NT)
        found = ((got[0:1] * 256.0 + got[1:2]) * total + (got[2:3] + b * rows)).astype(jnp.int32)
        amount = jnp.sum(mine_f[b : b + 1], axis=1, keepdims=True).astype(jnp.int32)
        slots_v[b : b + 1, :slot_max] = found
        slots_v[b : b + 1, slot_max:] = jnp.broadcast_to(amount, (1, slot_max))
    listing = pltpu.make_async_copy(slots_v, slots_s, list_sem)
    listing.start()

    code_row = feat[width + 1 : width + 2, :].astype(jnp.float32)
    hot[...] = jnp.where(
        lax.broadcasted_iota(jnp.int32, (coarse_total, total), 0).astype(jnp.float32) == code_row, 1.0, 0.0
    ).astype(jnp.bfloat16)
    sums = mm(feat[: width + PACK, :], hot[...], NT)
    count = sums[width : width + 1]
    average = sums[:width] / jnp.maximum(count, 1.0)
    filled = jnp.broadcast_to(count, (width, coarse_total)).T > 0
    new_coarse_ref[...] = jnp.where(filled, average.T, old_coarse_ref[...])
    pieces = thirds(average)
    ones = jnp.where(lax.broadcasted_iota(jnp.int32, (PACK, rows), 0) == 0, 1.0, 0.0).astype(jnp.bfloat16)
    for b in range(blocks):
        cols = slice(b * rows, (b + 1) * rows)
        near = whole(mm(pieces, hot[:, cols], NN))
        crs[:width, cols] = (feat[:width, cols].astype(jnp.float32) - near).astype(jnp.bfloat16)
        crs[width:, cols] = ones

    id_row = feat[width + 2 : width + 3, :].astype(jnp.float32) * 256.0 + feat[width + 3 : width + 4, :].astype(
        jnp.float32
    )
    id_col = jnp.broadcast_to(id_row, (128, total)).T
    for b in range(blocks):
        cols = slice(b * rows, (b + 1) * rows)
        same = jnp.concatenate(
            [
                jnp.where(id_col == id_row[:, at : at + 128], 1.0, 0.0).astype(jnp.bfloat16)
                for at in range(b * rows, (b + 1) * rows, 128)
            ],
            axis=1,
        )
        fine = mm(crs[...], same, NN)
        mean = fine[:width] / fine[width : width + 1]
        res[:, cols] = (crs[:width, cols].astype(jnp.float32) - mean).astype(jnp.bfloat16)
        mean_rows[cols, :] = mean.T
    residual_ref[...] = res[:, :rows].astype(jnp.float32).T.astype(jnp.bfloat16)

    listing.wait()
    load.wait()
    for b in range(blocks):

        def put(i, carry):
            entry = slots_s[b, i]
            table[pl.ds(entry // total, 1), :] = mean_rows[pl.ds(entry % total, 1), :]
            return carry

        lax.fori_loop(0, slots_s[b, slot_max], put, 0)
    store = pltpu.make_async_copy(table, new_fine_ref, out_sem)
    store.start()

    code_at = lax.broadcasted_iota(jnp.int32, (code_total, total), 0).astype(jnp.float32)
    ones_all = jnp.where(lax.broadcasted_iota(jnp.int32, (PACK, total), 0) == 0, 1.0, 0.0).astype(jnp.bfloat16)
    error = jnp.zeros((sub_width, rows), jnp.float32)
    for m in range(sub_dev):
        band = slice(m * sub_width, (m + 1) * sub_width)
        row = feat[width + PACK + m : width + PACK + m + 1, :].astype(jnp.float32)
        hot_m = jnp.where(code_at == row, 1.0, 0.0).astype(jnp.bfloat16)
        sums = mm(jnp.concatenate([res[band, :], ones_all], axis=0), hot_m, NT)
        count = sums[sub_width : sub_width + 1]
        average = sums[:sub_width] / jnp.maximum(count, 1.0)
        books[band, :] = average
        counts[band, :] = jnp.broadcast_to(count, (sub_width, code_total))
        near = whole(mm(thirds(average), hot_m[:, :rows], NN))
        differ = res[band, :rows].astype(jnp.float32) - near
        error = error + differ * differ
    error_ref[...] = jnp.sum(error, axis=0, keepdims=True)
    books[...] = books[...].T
    counts[...] = counts[...].T
    own = pl.ds(pl.multiple_of(me * share, share), share)
    new_book_ref[...] = jnp.where(counts[own, :] > 0, books[own, :], old_book_ref[...])
    store.wait()


def gather_blocks(block, count):
    def hop(value, pairs):
        return lax.ppermute(value, "rows", pairs)

    half = count // 2
    near = [block]
    for k in range(1, half):
        near.append(hop(block, [(i, (i + 2 * k) % count) for i in range(count)]))
    far = [hop(value, [(i, i ^ 1) for i in range(count)]) for value in near]
    return near + far


def gathered_shards(embeddings, coarse_ids, fine_ids, pq_codes, old_coarse, old_fine, old_codebook):
    blocks = lax.axis_size("rows")
    rows, width = embeddings.shape
    coarse_total = old_coarse.shape[0]
    fine_dev = old_fine.shape[0]
    sub_dev = pq_codes.shape[1]
    share = old_codebook.shape[0]
    code_total = share * blocks
    total = rows * blocks
    slot_max = max(4 * rows // blocks, 1)
    height = width + PACK + sub_dev
    block = pl.pallas_call(
        pack_kernel,
        out_shape=jax.ShapeDtypeStruct((height, rows), jnp.bfloat16),
    )(embeddings, coarse_ids.reshape(1, rows), fine_ids.reshape(1, rows), pq_codes)
    parts = gather_blocks(block, blocks)
    vmem = pl.BlockSpec(memory_space=pltpu.VMEM)
    hbm = pl.BlockSpec(memory_space=pltpu.HBM)
    new_coarse, new_fine, residual, new_book, error = pl.pallas_call(
        functools.partial(steps_kernel, blocks),
        out_shape=(
            jax.ShapeDtypeStruct(old_coarse.shape, jnp.float32),
            jax.ShapeDtypeStruct(old_fine.shape, jnp.float32),
            jax.ShapeDtypeStruct(embeddings.shape, jnp.bfloat16),
            jax.ShapeDtypeStruct(old_codebook.shape, jnp.float32),
            jax.ShapeDtypeStruct((1, rows), jnp.float32),
        ),
        in_specs=[vmem] * (blocks + 2) + [hbm],
        out_specs=(vmem, hbm, vmem, vmem, vmem),
        scratch_shapes=[
            pltpu.VMEM((fine_dev, width), jnp.float32),
            pltpu.VMEM((height, total), jnp.bfloat16),
            pltpu.VMEM((coarse_total, total), jnp.bfloat16),
            pltpu.VMEM((width + PACK, total), jnp.bfloat16),
            pltpu.VMEM((total, width), jnp.float32),
            pltpu.VMEM((width, total), jnp.bfloat16),
            pltpu.VMEM((width, code_total), jnp.float32),
            pltpu.VMEM((width, code_total), jnp.float32),
            pltpu.VMEM((blocks, 2 * slot_max), jnp.int32),
            pltpu.SMEM((blocks, 2 * slot_max), jnp.int32),
            pltpu.SemaphoreType.DMA,
            pltpu.SemaphoreType.DMA,
            pltpu.SemaphoreType.DMA,
        ],
        compiler_params=pltpu.CompilerParams(vmem_limit_bytes=48 * 2**20),
    )(*parts, old_coarse, old_codebook, old_fine)
    row_error = jnp.sum(lax.all_gather(error, "rep", axis=0, tiled=True), axis=0) / (width * lax.axis_size("rep"))
    return (new_coarse, new_fine, residual, new_book, row_error)


def fits(sizes):
    rows, width, blocks, fine_dev, sub_dev, code_total, coarse_total, fine_total = sizes
    digits = 256
    return (
        blocks % 2 == 0
        and rows * blocks <= fine_dev
        and rows % 128 == 0
        and rows <= digits
        and coarse_total <= digits
        and code_total <= digits
        and fine_total <= digits * digits
        and width == code_total
        and width // sub_dev == PACK
        and sub_dev % PACK == 0
        and (4 * rows // blocks) % 128 == 0
    )


def shards(*args):
    embeddings, _, _, pq_codes, old_coarse, old_fine, old_codebook = args
    blocks = lax.axis_size("rows")
    rows, width = embeddings.shape
    fine_dev = old_fine.shape[0]
    sizes = (
        rows,
        width,
        blocks,
        fine_dev,
        pq_codes.shape[1],
        old_codebook.shape[0] * blocks,
        old_coarse.shape[0],
        fine_dev * blocks,
    )
    return gathered_shards(*args) if fits(sizes) else exchange_shards(*args)


def solution(mesh):
    placed = (
        P("rows", "rep"),
        P("rows"),
        P("rows"),
        P("rows", "rep"),
        P(None, "rep"),
        P("rows", "rep"),
        P("rows", "rep"),
    )
    return jax.shard_map(
        shards,
        mesh=mesh,
        in_specs=placed,
        out_specs=(P(None, "rep"), P("rows", "rep"), P("rows", "rep"), P("rows", "rep"), P("rows")),
        check_vma=False,
    )
```

```python
import functools
import math

import jax
import jax.numpy as jnp
from jax import lax
from jax.experimental import pallas as pl
from jax.experimental.pallas import tpu as pltpu
from jax.sharding import PartitionSpec as P


def update_means(sums, counts, fallback):
    return jnp.where(counts[:, None] > 0, sums / jnp.maximum(counts, 1.0)[:, None], fallback)


def exchange_shards(embeddings, coarse_ids, fine_ids, pq_codes, old_coarse, old_fine, old_codebook):
    owner_rows = lax.axis_size("rows")
    row_total, width_dev = embeddings.shape
    coarse_total = old_coarse.shape[0]
    coarse_hot = coarse_ids[None, :] == jnp.arange(coarse_total, dtype=jnp.int32)[:, None]
    coarse_sum = jnp.dot(
        coarse_hot.astype(jnp.bfloat16), embeddings, preferred_element_type=jnp.float32
    )
    coarse_count = jnp.sum(coarse_hot, axis=1).astype(jnp.float32)
    coarse_sum, coarse_count = lax.psum((coarse_sum, coarse_count), "rows")
    new_coarse = update_means(coarse_sum, coarse_count, old_coarse)
    coarse_residual = (
        embeddings.astype(jnp.float32) - jnp.take(new_coarse, coarse_ids, axis=0)
    ).astype(jnp.bfloat16)
    fine_dev = old_fine.shape[0]
    capacity = 4 * row_total // owner_rows
    slot_total = owner_rows * capacity
    owner_ids = fine_ids // fine_dev
    local_ids = fine_ids % fine_dev
    owner_hot = (owner_ids[:, None] == jnp.arange(owner_rows, dtype=jnp.int32)[None, :]).astype(
        jnp.int32
    )
    rank_in = jnp.sum(jnp.cumsum(owner_hot, axis=0) * owner_hot, axis=1) - 1
    slot_of_row = owner_ids * capacity + rank_in
    row_of_slot = (
        jnp.full((slot_total,), row_total, jnp.int32)
        .at[slot_of_row]
        .set(jnp.arange(row_total, dtype=jnp.int32))
    )
    send_rows = jnp.take(coarse_residual, row_of_slot, axis=0, mode="fill", fill_value=0).reshape(
        owner_rows, capacity, width_dev
    )
    send_ids = (
        jnp.full((slot_total,), -1, jnp.int32)
        .at[slot_of_row]
        .set(local_ids)
        .reshape(owner_rows, capacity)
    )
    recv_rows, recv_ids = (
        lax.all_to_all(send_rows, "rows", split_axis=0, concat_axis=0, tiled=True),
        lax.all_to_all(send_ids, "rows", split_axis=0, concat_axis=0, tiled=True),
    )
    rows_flat = recv_rows.reshape(slot_total, width_dev)
    ids_flat = recv_ids.reshape(slot_total)
    block_size = math.gcd(slot_total, 2048)
    fine_range = jnp.arange(fine_dev, dtype=jnp.int32)

    def fine_step(running, pieces):
        sums, counts = running
        block_rows, block_ids = pieces
        one_hot = block_ids[None, :] == fine_range[:, None]
        sums = sums + jnp.dot(
            one_hot.astype(jnp.bfloat16), block_rows, preferred_element_type=jnp.float32
        )
        counts = counts + jnp.sum(one_hot, axis=1).astype(jnp.float32)
        return ((sums, counts), None)

    start_fine = (
        jnp.zeros((fine_dev, width_dev), jnp.float32),
        jnp.zeros((fine_dev,), jnp.float32),
    )
    (fine_sum, fine_count), _ = lax.scan(
        fine_step,
        start_fine,
        (
            rows_flat.reshape(slot_total // block_size, block_size, width_dev),
            ids_flat.reshape(slot_total // block_size, block_size),
        ),
    )
    new_fine = update_means(fine_sum, fine_count, old_fine)
    safe_ids = jnp.maximum(ids_flat, 0)
    at_owner = (rows_flat.astype(jnp.float32) - jnp.take(new_fine, safe_ids, axis=0)).astype(
        jnp.bfloat16
    )
    returned = lax.all_to_all(
        at_owner.reshape(owner_rows, capacity, width_dev),
        "rows",
        split_axis=0,
        concat_axis=0,
        tiled=True,
    ).reshape(slot_total, width_dev)
    residual = jnp.take(returned, slot_of_row, axis=0)
    sub_dev = pq_codes.shape[1]
    sub_width = width_dev // sub_dev
    share_codes = old_codebook.shape[0]
    book_rows = share_codes * owner_rows
    code_block = math.gcd(row_total, 512)
    code_range = jnp.arange(book_rows, dtype=jnp.int32)

    def code_step(running, pieces):
        sums, counts = running
        block_rows, block_codes = pieces
        one_hot = block_codes.T[:, None, :] == code_range[None, :, None]
        split_rows = block_rows.reshape(code_block, sub_dev, sub_width)
        sums = sums + jnp.einsum(
            "mkn,nmd->kmd",
            one_hot.astype(jnp.bfloat16),
            split_rows,
            preferred_element_type=jnp.float32,
        )
        counts = counts + jnp.sum(one_hot, axis=2).T.astype(jnp.float32)
        return ((sums, counts), None)

    start_code = (
        jnp.zeros((book_rows, sub_dev, sub_width), jnp.float32),
        jnp.zeros((book_rows, sub_dev), jnp.float32),
    )
    (code_sum, code_count), _ = lax.scan(
        code_step,
        start_code,
        (
            residual.reshape(row_total // code_block, code_block, width_dev),
            pq_codes.reshape(row_total // code_block, code_block, sub_dev),
        ),
    )
    code_sum = code_sum.reshape(book_rows, width_dev)
    code_sum, code_count = lax.psum((code_sum, code_count), "rows")
    column_count = jnp.repeat(code_count, sub_width, axis=1)
    averages = code_sum / jnp.maximum(column_count, 1.0)
    first_code = lax.axis_index("rows") * share_codes
    own_count = lax.dynamic_slice_in_dim(column_count, first_code, share_codes, 0)
    own_average = lax.dynamic_slice_in_dim(averages, first_code, share_codes, 0)
    new_codebook = jnp.where(own_count > 0, own_average, old_codebook)
    book_view = averages.reshape(book_rows, sub_dev, sub_width)
    rebuilt = book_view[pq_codes, jnp.arange(sub_dev, dtype=jnp.int32)[None, :]].reshape(
        row_total, width_dev
    )
    differ = residual.astype(jnp.float32) - rebuilt
    partial_error = jnp.sum(differ * differ, axis=1)
    row_error = lax.psum(partial_error, "rep") / (width_dev * lax.axis_size("rep"))
    return (new_coarse, new_fine, residual, new_codebook, row_error)


PACK = 16
NN = (((1,), (0,)), ((), ()))
NT = (((1,), (1,)), ((), ()))
GROUP = 8


def mm(left, right, dims):
    return lax.dot_general(left, right, dims, preferred_element_type=jnp.float32)


def thirds(value):
    high = value.astype(jnp.bfloat16)
    rest = value - high.astype(jnp.float32)
    middle = rest.astype(jnp.bfloat16)
    low = (rest - middle.astype(jnp.float32)).astype(jnp.bfloat16)
    return jnp.concatenate([high, middle, low], axis=0)


def whole(pieces):
    size = pieces.shape[0] // 3
    return (pieces[:size] + pieces[size : 2 * size]) + pieces[2 * size :]


def pack_kernel(emb_ref, coarse_ref, fine_ref, codes_ref, out_ref):
    width = emb_ref.shape[1]
    rows = emb_ref.shape[0]
    out_ref[:width] = emb_ref[...].T
    fine = fine_ref[...]
    place = lax.broadcasted_iota(jnp.int32, (PACK, rows), 0)
    ids = jnp.where(
        place == 0,
        1,
        jnp.where(
            place == 1, coarse_ref[...], jnp.where(place == 2, fine >> 8, jnp.where(place == 3, fine & 255, 0))
        ),
    )
    out_ref[width : width + PACK] = ids.astype(jnp.float32).astype(jnp.bfloat16)
    out_ref[width + PACK :] = codes_ref[...].astype(jnp.float32).astype(jnp.bfloat16)


def stage_kernel(coarse_ref, book_ref, coarse_out, book_out):
    coarse_out[...] = coarse_ref[...]
    book_out[...] = book_ref[...]


def steps_kernel(blocks, *refs):
    parts = refs[:blocks]
    (old_coarse_ref, old_book_ref, old_fine_ref) = refs[blocks : blocks + 3]
    (new_coarse_ref, new_fine_ref, residual_ref, new_book_ref, error_ref) = refs[blocks + 3 : blocks + 8]
    (table, feat, crs, mean_rows, res, books, counts, columns, slots_v, slots_s) = refs[
        blocks + 8 : blocks + 18
    ]
    (in_sem, out_sem, list_sem) = refs[blocks + 18 :]
    coarse_total, width = old_coarse_ref.shape
    share = old_book_ref.shape[0]
    fine_dev = old_fine_ref.shape[0]
    rows = parts[0].shape[1]
    total = rows * blocks
    sub_dev = parts[0].shape[0] - width - PACK
    sub_width = width // sub_dev
    code_total = share * blocks
    me = lax.axis_index("rows")

    load = pltpu.make_async_copy(old_fine_ref, table.at[:fine_dev], in_sem)
    load.start()
    for b in range(blocks):
        feat[:, b * rows : (b + 1) * rows] = parts[b][...]

    steps = slots_s.shape[0] // blocks
    slot_max = steps * GROUP
    digits = [
        jnp.concatenate([parts[b][width + 2 + d : width + 3 + d].astype(jnp.float32) for b in range(blocks)], axis=0)
        for d in range(2)
    ]
    ids8 = (digits[0] * 256.0 + digits[1]).astype(jnp.int32)
    local8 = ids8 - me * fine_dev
    mine = jnp.logical_and(local8 >= 0, local8 < fine_dev)
    mine_f = jnp.where(mine, 1.0, 0.0)
    earlier = lax.broadcasted_iota(jnp.int32, (rows, rows), 0) < lax.broadcasted_iota(jnp.int32, (rows, rows), 1)
    rank = mm(mine_f.astype(jnp.bfloat16), jnp.where(earlier, 1.0, 0.0).astype(jnp.bfloat16), NN)
    rank = jnp.where(mine, rank.astype(jnp.int32), -1)
    local8 = jnp.where(mine, local8, 0)
    lane = lax.broadcasted_iota(jnp.int32, (1, rows), 1)
    place = lax.broadcasted_iota(jnp.int32, (slot_max, rows), 0)
    slot_at = (place % steps) * GROUP + place // steps
    list_lane = lax.broadcasted_iota(jnp.int32, (steps, slots_s.shape[1]), 1)
    for b in range(blocks):
        pick = jnp.where(slot_at == rank[b : b + 1], 1.0, 0.0).astype(jnp.bfloat16)
        mine_b = local8[b : b + 1]
        values = jnp.concatenate(
            [(mine_b >> 8).astype(jnp.float32), (mine_b & 255).astype(jnp.float32), lane.astype(jnp.float32)]
            + [jnp.zeros((5, rows), jnp.float32)],
            axis=0,
        ).astype(jnp.bfloat16)
        got = mm(pick, values, NT)
        amount = jnp.sum(mine_f[b : b + 1], axis=1, keepdims=True).astype(jnp.int32)
        goal = (got[:, 0:1] * 256.0 + got[:, 1:2]).astype(jnp.int32)
        goal = jnp.where(slot_at[:, :1] < amount, goal, fine_dev)
        source = got[:, 2:3].astype(jnp.int32) + b * rows
        listed = jnp.broadcast_to((amount + GROUP - 1) // GROUP, list_lane.shape)
        for k in range(GROUP):
            part = slice(k * steps, (k + 1) * steps)
            listed = jnp.where(list_lane == k, goal[part], listed)
            listed = jnp.where(list_lane == GROUP + k, source[part], listed)
        slots_v[b * steps : (b + 1) * steps, :] = listed
    listing = pltpu.make_async_copy(slots_v, slots_s, list_sem)
    listing.start()

    digit_col = feat[width : width + PACK, :].astype(jnp.float32).T
    code_lane = lax.broadcasted_iota(jnp.int32, (1, coarse_total), 1).astype(jnp.float32)
    hot = jnp.where(digit_col[:, 1:2] == code_lane, 1.0, 0.0).astype(jnp.bfloat16)
    sums = mm(feat[: width + PACK, :], hot, NN)
    count = sums[width : width + 1]
    average = sums[:width] / jnp.maximum(count, 1.0)
    filled = jnp.broadcast_to(count, (width, coarse_total)).T > 0
    new_coarse_ref[...] = jnp.where(filled, average.T, old_coarse_ref[...])
    coarse_at = lax.broadcasted_iota(jnp.int32, (coarse_total, rows), 0).astype(jnp.float32)
    pieces = thirds(average)
    ones = jnp.where(lax.broadcasted_iota(jnp.int32, (PACK, rows), 0) == 0, 1.0, 0.0).astype(jnp.bfloat16)
    for b in range(blocks):
        cols = slice(b * rows, (b + 1) * rows)
        code_row = feat[width + 1 : width + 2, cols].astype(jnp.float32)
        hot = jnp.where(coarse_at == code_row, 1.0, 0.0).astype(jnp.bfloat16)
        near = whole(mm(pieces, hot, NN))
        crs[:width, cols] = (feat[:width, cols].astype(jnp.float32) - near).astype(jnp.bfloat16)
        crs[width:, cols] = ones

    id_row = feat[width + 2 : width + 3, :].astype(jnp.float32) * 256.0 + feat[width + 3 : width + 4, :].astype(
        jnp.float32
    )
    id_col = jnp.broadcast_to(digit_col[:, 2:3] * 256.0 + digit_col[:, 3:4], (total, 128))
    for b in range(blocks):
        cols = slice(b * rows, (b + 1) * rows)
        same = jnp.concatenate(
            [
                jnp.where(id_col == id_row[:, at : at + 128], 1.0, 0.0).astype(jnp.bfloat16)
                for at in range(b * rows, (b + 1) * rows, 128)
            ],
            axis=1,
        )
        fine = mm(crs[...], same, NN)
        mean = fine[:width] / fine[width : width + 1]
        res[:, cols] = (crs[:width, cols].astype(jnp.float32) - mean).astype(jnp.bfloat16)
        mean_rows[cols, 0, :] = mean.T
    residual_ref[...] = res[:, :rows].astype(jnp.float32).T.astype(jnp.bfloat16)

    listing.wait()
    load.wait()
    for b in range(blocks):

        def put(i, carry):
            means = [mean_rows[slots_s[i, GROUP + k]] for k in range(GROUP)]
            for k in range(GROUP):
                table[pl.ds(slots_s[i, k], 1), :] = means[k]
            return carry

        lax.fori_loop(b * steps, b * steps + slots_s[b * steps, 2 * GROUP], put, 0)
    store = pltpu.make_async_copy(table.at[:fine_dev], new_fine_ref, out_sem)
    store.start()

    columns[...] = feat[width + PACK :, :].astype(jnp.float32).T
    code_at = lax.broadcasted_iota(jnp.int32, (code_total, rows), 0).astype(jnp.float32)
    code_lane = lax.broadcasted_iota(jnp.int32, (1, code_total), 1).astype(jnp.float32)
    ones_all = jnp.where(lax.broadcasted_iota(jnp.int32, (PACK, total), 0) == 0, 1.0, 0.0).astype(jnp.bfloat16)
    error = jnp.zeros((sub_width, rows), jnp.float32)
    for m in range(sub_dev):
        band = slice(m * sub_width, (m + 1) * sub_width)
        hot_m = jnp.where(columns[:, m : m + 1] == code_lane, 1.0, 0.0).astype(jnp.bfloat16)
        sums = mm(jnp.concatenate([res[band, :], ones_all], axis=0), hot_m, NN)
        count = sums[sub_width : sub_width + 1]
        average = sums[:sub_width] / jnp.maximum(count, 1.0)
        books[band, :] = average
        counts[band, :] = jnp.broadcast_to(count, (sub_width, code_total))
        row = feat[width + PACK + m : width + PACK + m + 1, :rows].astype(jnp.float32)
        near = whole(mm(thirds(average), jnp.where(code_at == row, 1.0, 0.0).astype(jnp.bfloat16), NN))
        differ = res[band, :rows].astype(jnp.float32) - near
        error = error + differ * differ
    error_ref[...] = jnp.sum(error, axis=0, keepdims=True)
    books[...] = books[...].T
    counts[...] = counts[...].T
    own = pl.ds(pl.multiple_of(me * share, share), share)
    new_book_ref[...] = jnp.where(counts[own, :] > 0, books[own, :], old_book_ref[...])
    store.wait()


def gather_blocks(block, count):
    def hop(value, pairs):
        return lax.ppermute(value, "rows", pairs)

    half = count // 2
    near = [block]
    for k in range(1, half):
        near.append(hop(block, [(i, (i + 2 * k) % count) for i in range(count)]))
    far = [hop(value, [(i, i ^ 1) for i in range(count)]) for value in near]
    return near + far


def gathered_shards(embeddings, coarse_ids, fine_ids, pq_codes, old_coarse, old_fine, old_codebook):
    blocks = lax.axis_size("rows")
    rows, width = embeddings.shape
    coarse_total = old_coarse.shape[0]
    fine_dev = old_fine.shape[0]
    sub_dev = pq_codes.shape[1]
    share = old_codebook.shape[0]
    code_total = share * blocks
    total = rows * blocks
    slot_max = max(4 * rows // blocks, 1)
    height = width + PACK + sub_dev
    block = pl.pallas_call(
        pack_kernel,
        out_shape=pltpu.VMEM((height, rows), jnp.bfloat16),
    )(embeddings, coarse_ids.reshape(1, rows), fine_ids.reshape(1, rows), pq_codes.T)
    parts = gather_blocks(block, blocks)
    vmem = pl.BlockSpec(memory_space=pltpu.VMEM)
    coarse_near, book_near = pl.pallas_call(
        stage_kernel,
        out_shape=(pltpu.VMEM(old_coarse.shape, jnp.float32), pltpu.VMEM(old_codebook.shape, jnp.float32)),
        in_specs=[vmem] * 2,
        cost_estimate=pl.CostEstimate(flops=10**6, bytes_accessed=10**6, transcendentals=0),
    )(old_coarse, old_codebook)
    hbm = pl.BlockSpec(memory_space=pltpu.HBM)
    new_coarse, new_fine, residual, new_book, error = pl.pallas_call(
        functools.partial(steps_kernel, blocks),
        out_shape=(
            jax.ShapeDtypeStruct(old_coarse.shape, jnp.float32),
            jax.ShapeDtypeStruct(old_fine.shape, jnp.float32),
            jax.ShapeDtypeStruct(embeddings.shape, jnp.bfloat16),
            jax.ShapeDtypeStruct(old_codebook.shape, jnp.float32),
            jax.ShapeDtypeStruct((1, rows), jnp.float32),
        ),
        in_specs=[vmem] * (blocks + 2) + [hbm],
        out_specs=(vmem, hbm, vmem, vmem, vmem),
        scratch_shapes=[
            pltpu.VMEM((fine_dev + GROUP, width), jnp.float32),
            pltpu.VMEM((height, total), jnp.bfloat16),
            pltpu.VMEM((width + PACK, total), jnp.bfloat16),
            pltpu.VMEM((total, 1, width), jnp.float32),
            pltpu.VMEM((width, total), jnp.bfloat16),
            pltpu.VMEM((width, code_total), jnp.float32),
            pltpu.VMEM((width, code_total), jnp.float32),
            pltpu.VMEM((total, sub_dev), jnp.float32),
            pltpu.VMEM((blocks * slot_max // GROUP, 128), jnp.int32),
            pltpu.SMEM((blocks * slot_max // GROUP, 128), jnp.int32),
        ]
        + [pltpu.SemaphoreType.DMA] * 3,
        compiler_params=pltpu.CompilerParams(vmem_limit_bytes=48 * 2**20),
    )(*parts, coarse_near, book_near, old_fine)
    row_error = jnp.sum(lax.all_gather(error, "rep", axis=0, tiled=True), axis=0) / (width * lax.axis_size("rep"))
    return (new_coarse, new_fine, residual, new_book, row_error)


def fits(sizes):
    rows, width, blocks, fine_dev, sub_dev, code_total, coarse_total, fine_total = sizes
    digits = 256
    return (
        blocks % 2 == 0
        and rows * blocks <= fine_dev
        and rows % 128 == 0
        and rows <= digits
        and coarse_total <= digits
        and code_total <= digits
        and fine_total <= digits * digits
        and width == code_total
        and width // sub_dev == PACK
        and sub_dev % PACK == 0
        and (4 * rows // blocks) % 128 == 0
    )


def shards(*args):
    embeddings, _, _, pq_codes, old_coarse, old_fine, old_codebook = args
    blocks = lax.axis_size("rows")
    rows, width = embeddings.shape
    fine_dev = old_fine.shape[0]
    sizes = (
        rows,
        width,
        blocks,
        fine_dev,
        pq_codes.shape[1],
        old_codebook.shape[0] * blocks,
        old_coarse.shape[0],
        fine_dev * blocks,
    )
    return gathered_shards(*args) if fits(sizes) else exchange_shards(*args)


def solution(mesh):
    placed = (
        P("rows", "rep"),
        P("rows"),
        P("rows"),
        P("rows", "rep"),
        P(None, "rep"),
        P("rows", "rep"),
        P("rows", "rep"),
    )
    return jax.shard_map(
        shards,
        mesh=mesh,
        in_specs=placed,
        out_specs=(P(None, "rep"), P("rows", "rep"), P("rows", "rep"), P("rows", "rep"), P("rows")),
        check_vma=False,
    )
```

```python
import functools
import math

import jax
import jax.numpy as jnp
from jax import lax
from jax.experimental import pallas as pl
from jax.experimental.pallas import tpu as pltpu
from jax.sharding import PartitionSpec as P


def update_means(sums, counts, fallback):
    return jnp.where(counts[:, None] > 0, sums / jnp.maximum(counts, 1.0)[:, None], fallback)


def exchange_shards(embeddings, coarse_ids, fine_ids, pq_codes, old_coarse, old_fine, old_codebook):
    owner_rows = lax.axis_size("rows")
    row_total, width_dev = embeddings.shape
    coarse_total = old_coarse.shape[0]
    coarse_hot = coarse_ids[None, :] == jnp.arange(coarse_total, dtype=jnp.int32)[:, None]
    coarse_sum = jnp.dot(
        coarse_hot.astype(jnp.bfloat16), embeddings, preferred_element_type=jnp.float32
    )
    coarse_count = jnp.sum(coarse_hot, axis=1).astype(jnp.float32)
    coarse_sum, coarse_count = lax.psum((coarse_sum, coarse_count), "rows")
    new_coarse = update_means(coarse_sum, coarse_count, old_coarse)
    coarse_residual = (
        embeddings.astype(jnp.float32) - jnp.take(new_coarse, coarse_ids, axis=0)
    ).astype(jnp.bfloat16)
    fine_dev = old_fine.shape[0]
    capacity = 4 * row_total // owner_rows
    slot_total = owner_rows * capacity
    owner_ids = fine_ids // fine_dev
    local_ids = fine_ids % fine_dev
    owner_hot = (owner_ids[:, None] == jnp.arange(owner_rows, dtype=jnp.int32)[None, :]).astype(
        jnp.int32
    )
    rank_in = jnp.sum(jnp.cumsum(owner_hot, axis=0) * owner_hot, axis=1) - 1
    slot_of_row = owner_ids * capacity + rank_in
    row_of_slot = (
        jnp.full((slot_total,), row_total, jnp.int32)
        .at[slot_of_row]
        .set(jnp.arange(row_total, dtype=jnp.int32))
    )
    send_rows = jnp.take(coarse_residual, row_of_slot, axis=0, mode="fill", fill_value=0).reshape(
        owner_rows, capacity, width_dev
    )
    send_ids = (
        jnp.full((slot_total,), -1, jnp.int32)
        .at[slot_of_row]
        .set(local_ids)
        .reshape(owner_rows, capacity)
    )
    recv_rows, recv_ids = (
        lax.all_to_all(send_rows, "rows", split_axis=0, concat_axis=0, tiled=True),
        lax.all_to_all(send_ids, "rows", split_axis=0, concat_axis=0, tiled=True),
    )
    rows_flat = recv_rows.reshape(slot_total, width_dev)
    ids_flat = recv_ids.reshape(slot_total)
    block_size = math.gcd(slot_total, 2048)
    fine_range = jnp.arange(fine_dev, dtype=jnp.int32)

    def fine_step(running, pieces):
        sums, counts = running
        block_rows, block_ids = pieces
        one_hot = block_ids[None, :] == fine_range[:, None]
        sums = sums + jnp.dot(
            one_hot.astype(jnp.bfloat16), block_rows, preferred_element_type=jnp.float32
        )
        counts = counts + jnp.sum(one_hot, axis=1).astype(jnp.float32)
        return ((sums, counts), None)

    start_fine = (
        jnp.zeros((fine_dev, width_dev), jnp.float32),
        jnp.zeros((fine_dev,), jnp.float32),
    )
    (fine_sum, fine_count), _ = lax.scan(
        fine_step,
        start_fine,
        (
            rows_flat.reshape(slot_total // block_size, block_size, width_dev),
            ids_flat.reshape(slot_total // block_size, block_size),
        ),
    )
    new_fine = update_means(fine_sum, fine_count, old_fine)
    safe_ids = jnp.maximum(ids_flat, 0)
    at_owner = (rows_flat.astype(jnp.float32) - jnp.take(new_fine, safe_ids, axis=0)).astype(
        jnp.bfloat16
    )
    returned = lax.all_to_all(
        at_owner.reshape(owner_rows, capacity, width_dev),
        "rows",
        split_axis=0,
        concat_axis=0,
        tiled=True,
    ).reshape(slot_total, width_dev)
    residual = jnp.take(returned, slot_of_row, axis=0)
    sub_dev = pq_codes.shape[1]
    sub_width = width_dev // sub_dev
    share_codes = old_codebook.shape[0]
    book_rows = share_codes * owner_rows
    code_block = math.gcd(row_total, 512)
    code_range = jnp.arange(book_rows, dtype=jnp.int32)

    def code_step(running, pieces):
        sums, counts = running
        block_rows, block_codes = pieces
        one_hot = block_codes.T[:, None, :] == code_range[None, :, None]
        split_rows = block_rows.reshape(code_block, sub_dev, sub_width)
        sums = sums + jnp.einsum(
            "mkn,nmd->kmd",
            one_hot.astype(jnp.bfloat16),
            split_rows,
            preferred_element_type=jnp.float32,
        )
        counts = counts + jnp.sum(one_hot, axis=2).T.astype(jnp.float32)
        return ((sums, counts), None)

    start_code = (
        jnp.zeros((book_rows, sub_dev, sub_width), jnp.float32),
        jnp.zeros((book_rows, sub_dev), jnp.float32),
    )
    (code_sum, code_count), _ = lax.scan(
        code_step,
        start_code,
        (
            residual.reshape(row_total // code_block, code_block, width_dev),
            pq_codes.reshape(row_total // code_block, code_block, sub_dev),
        ),
    )
    code_sum = code_sum.reshape(book_rows, width_dev)
    code_sum, code_count = lax.psum((code_sum, code_count), "rows")
    column_count = jnp.repeat(code_count, sub_width, axis=1)
    averages = code_sum / jnp.maximum(column_count, 1.0)
    first_code = lax.axis_index("rows") * share_codes
    own_count = lax.dynamic_slice_in_dim(column_count, first_code, share_codes, 0)
    own_average = lax.dynamic_slice_in_dim(averages, first_code, share_codes, 0)
    new_codebook = jnp.where(own_count > 0, own_average, old_codebook)
    book_view = averages.reshape(book_rows, sub_dev, sub_width)
    rebuilt = book_view[pq_codes, jnp.arange(sub_dev, dtype=jnp.int32)[None, :]].reshape(
        row_total, width_dev
    )
    differ = residual.astype(jnp.float32) - rebuilt
    partial_error = jnp.sum(differ * differ, axis=1)
    row_error = lax.psum(partial_error, "rep") / (width_dev * lax.axis_size("rep"))
    return (new_coarse, new_fine, residual, new_codebook, row_error)


PACK = 16
NN = (((1,), (0,)), ((), ()))
NT = (((1,), (1,)), ((), ()))
GROUP = 8


def mm(left, right, dims):
    return lax.dot_general(left, right, dims, preferred_element_type=jnp.float32)


def thirds(value):
    high = value.astype(jnp.bfloat16)
    rest = value - high.astype(jnp.float32)
    middle = rest.astype(jnp.bfloat16)
    low = (rest - middle.astype(jnp.float32)).astype(jnp.bfloat16)
    return jnp.concatenate([high, middle, low], axis=0)


def whole(pieces):
    size = pieces.shape[0] // 3
    return (pieces[:size] + pieces[size : 2 * size]) + pieces[2 * size :]


def pack_kernel(emb_ref, coarse_ref, fine_ref, codes_ref, out_ref):
    width = emb_ref.shape[1]
    rows = emb_ref.shape[0]
    out_ref[:width] = emb_ref[...].T
    fine = fine_ref[...]
    place = lax.broadcasted_iota(jnp.int32, (PACK, rows), 0)
    ids = jnp.where(
        place == 0,
        1,
        jnp.where(
            place == 1, coarse_ref[...], jnp.where(place == 2, fine >> 8, jnp.where(place == 3, fine & 255, 0))
        ),
    )
    out_ref[width : width + PACK] = ids.astype(jnp.float32).astype(jnp.bfloat16)
    out_ref[width + PACK :] = codes_ref[...].astype(jnp.float32).astype(jnp.bfloat16)


def stage_kernel(coarse_ref, book_ref, coarse_out, book_out):
    coarse_out[...] = coarse_ref[...]
    book_out[...] = book_ref[...]


def steps_kernel(blocks, *refs):
    parts = refs[:blocks]
    (old_coarse_ref, old_book_ref, old_fine_ref) = refs[blocks : blocks + 3]
    (new_coarse_ref, new_fine_ref, residual_ref, new_book_ref, error_ref) = refs[blocks + 3 : blocks + 8]
    (table, feat, crs, mean_rows, res, books, counts, columns, slots_v, slots_s) = refs[
        blocks + 8 : blocks + 18
    ]
    (in_sem, out_sem, list_sem) = refs[blocks + 18 :]
    coarse_total, width = old_coarse_ref.shape
    share = old_book_ref.shape[0]
    fine_dev = old_fine_ref.shape[0]
    rows = parts[0].shape[1]
    total = rows * blocks
    sub_dev = parts[0].shape[0] - width - PACK
    sub_width = width // sub_dev
    code_total = share * blocks
    me = lax.axis_index("rows")

    load = pltpu.make_async_copy(old_fine_ref, table.at[:fine_dev], in_sem)
    load.start()
    for b in range(blocks):
        feat[:, b * rows : (b + 1) * rows] = parts[b][...]

    steps = slots_s.shape[0] // blocks
    slot_max = steps * GROUP
    digits = [
        jnp.concatenate([parts[b][width + 2 + d : width + 3 + d].astype(jnp.float32) for b in range(blocks)], axis=0)
        for d in range(2)
    ]
    ids8 = (digits[0] * 256.0 + digits[1]).astype(jnp.int32)
    local8 = ids8 - me * fine_dev
    mine = jnp.logical_and(local8 >= 0, local8 < fine_dev)
    mine_f = jnp.where(mine, 1.0, 0.0)
    earlier = lax.broadcasted_iota(jnp.int32, (rows, rows), 0) < lax.broadcasted_iota(jnp.int32, (rows, rows), 1)
    rank = mm(mine_f.astype(jnp.bfloat16), jnp.where(earlier, 1.0, 0.0).astype(jnp.bfloat16), NN)
    rank = jnp.where(mine, rank.astype(jnp.int32), -1)
    local8 = jnp.where(mine, local8, 0)
    lane = lax.broadcasted_iota(jnp.int32, (1, rows), 1)
    place = lax.broadcasted_iota(jnp.int32, (slot_max, rows), 0)
    slot_at = (place % steps) * GROUP + place // steps
    list_lane = lax.broadcasted_iota(jnp.int32, (steps, slots_s.shape[1]), 1)
    for b in range(blocks):
        pick = jnp.where(slot_at == rank[b : b + 1], 1.0, 0.0).astype(jnp.bfloat16)
        mine_b = local8[b : b + 1]
        values = jnp.concatenate(
            [(mine_b >> 8).astype(jnp.float32), (mine_b & 255).astype(jnp.float32), lane.astype(jnp.float32)]
            + [jnp.zeros((5, rows), jnp.float32)],
            axis=0,
        ).astype(jnp.bfloat16)
        got = mm(pick, values, NT)
        amount = jnp.sum(mine_f[b : b + 1], axis=1, keepdims=True).astype(jnp.int32)
        goal = (got[:, 0:1] * 256.0 + got[:, 1:2]).astype(jnp.int32)
        goal = jnp.where(slot_at[:, :1] < amount, goal, fine_dev)
        source = got[:, 2:3].astype(jnp.int32) + b * rows
        listed = jnp.broadcast_to((amount + GROUP - 1) // GROUP, list_lane.shape)
        for k in range(GROUP):
            part = slice(k * steps, (k + 1) * steps)
            listed = jnp.where(list_lane == k, goal[part], listed)
            listed = jnp.where(list_lane == GROUP + k, source[part], listed)
        slots_v[b * steps : (b + 1) * steps, :] = listed
    listing = pltpu.make_async_copy(slots_v, slots_s, list_sem)
    listing.start()

    digit_col = feat[width : width + PACK, :].astype(jnp.float32).T
    code_lane = lax.broadcasted_iota(jnp.int32, (1, coarse_total), 1).astype(jnp.float32)
    hot = jnp.where(digit_col[:, 1:2] == code_lane, 1.0, 0.0).astype(jnp.bfloat16)
    sums = mm(feat[: width + PACK, :], hot, NN)
    count = sums[width : width + 1]
    average = sums[:width] / jnp.maximum(count, 1.0)
    filled = jnp.broadcast_to(count, (width, coarse_total)).T > 0
    new_coarse_ref[...] = jnp.where(filled, average.T, old_coarse_ref[...])
    coarse_at = lax.broadcasted_iota(jnp.int32, (coarse_total, rows), 0).astype(jnp.float32)
    pieces = thirds(average)
    ones = jnp.where(lax.broadcasted_iota(jnp.int32, (PACK, rows), 0) == 0, 1.0, 0.0).astype(jnp.bfloat16)
    for b in range(blocks):
        cols = slice(b * rows, (b + 1) * rows)
        code_row = feat[width + 1 : width + 2, cols].astype(jnp.float32)
        hot = jnp.where(coarse_at == code_row, 1.0, 0.0).astype(jnp.bfloat16)
        near = whole(mm(pieces, hot, NN))
        crs[:width, cols] = (feat[:width, cols].astype(jnp.float32) - near).astype(jnp.bfloat16)
        crs[width:, cols] = ones

    id_row = feat[width + 2 : width + 3, :].astype(jnp.float32) * 256.0 + feat[width + 3 : width + 4, :].astype(
        jnp.float32
    )
    id_col = jnp.broadcast_to(digit_col[:, 2:3] * 256.0 + digit_col[:, 3:4], (total, 128))
    for b in range(blocks):
        cols = slice(b * rows, (b + 1) * rows)
        same = jnp.concatenate(
            [
                jnp.where(id_col == id_row[:, at : at + 128], 1.0, 0.0).astype(jnp.bfloat16)
                for at in range(b * rows, (b + 1) * rows, 128)
            ],
            axis=1,
        )
        fine = mm(crs[...], same, NN)
        mean = fine[:width] / fine[width : width + 1]
        res[:, cols] = (crs[:width, cols].astype(jnp.float32) - mean).astype(jnp.bfloat16)
        mean_rows[cols, 0, :] = mean.T
    residual_ref[...] = res[:, :rows].astype(jnp.float32).T.astype(jnp.bfloat16)

    listing.wait()
    load.wait()
    for b in range(blocks):

        def put(i, carry):
            means = [mean_rows[slots_s[i, GROUP + k]] for k in range(GROUP)]
            for k in range(GROUP):
                table[pl.ds(slots_s[i, k], 1), :] = means[k]
            return carry

        lax.fori_loop(b * steps, b * steps + slots_s[b * steps, 2 * GROUP], put, 0)
    store = pltpu.make_async_copy(table.at[:fine_dev], new_fine_ref, out_sem)
    store.start()

    columns[...] = feat[width + PACK :, :].astype(jnp.float32).T
    code_at = lax.broadcasted_iota(jnp.int32, (code_total, rows), 0).astype(jnp.float32)
    code_lane = lax.broadcasted_iota(jnp.int32, (1, code_total), 1).astype(jnp.float32)
    ones_all = jnp.where(lax.broadcasted_iota(jnp.int32, (PACK, total), 0) == 0, 1.0, 0.0).astype(jnp.bfloat16)
    error = jnp.zeros((sub_width, rows), jnp.float32)
    for m in range(sub_dev):
        band = slice(m * sub_width, (m + 1) * sub_width)
        hot_m = jnp.where(columns[:, m : m + 1] == code_lane, 1.0, 0.0).astype(jnp.bfloat16)
        sums = mm(jnp.concatenate([res[band, :], ones_all], axis=0), hot_m, NN)
        count = sums[sub_width : sub_width + 1]
        average = sums[:sub_width] / jnp.maximum(count, 1.0)
        books[band, :] = average
        counts[band, :] = jnp.broadcast_to(count, (sub_width, code_total))
        row = feat[width + PACK + m : width + PACK + m + 1, :rows].astype(jnp.float32)
        near = whole(mm(thirds(average), jnp.where(code_at == row, 1.0, 0.0).astype(jnp.bfloat16), NN))
        differ = res[band, :rows].astype(jnp.float32) - near
        error = error + differ * differ
    error_ref[...] = jnp.sum(error, axis=0, keepdims=True)
    books[...] = books[...].T
    counts[...] = counts[...].T
    own = pl.ds(pl.multiple_of(me * share, share), share)
    new_book_ref[...] = jnp.where(counts[own, :] > 0, books[own, :], old_book_ref[...])
    store.wait()


def gather_blocks(block, count):
    def flip(value, step):
        return lax.ppermute(value, "rows", [(i, i ^ step) for i in range(count)])

    near = {0: block}
    step = count // 2
    while step > 1:
        near.update({at + step: flip(value, step) for at, value in list(near.items())})
        step //= 2
    last, top = count - 2, count // 2
    far = {at: flip(value, 1) for at, value in near.items() if at != last or count < 4}
    if count >= 4:
        far[last] = flip(far[last - top], top)
    order = sorted(near)
    return [near[at] for at in order] + [far[at] for at in order]


def gathered_shards(embeddings, coarse_ids, fine_ids, pq_codes, old_coarse, old_fine, old_codebook):
    blocks = lax.axis_size("rows")
    rows, width = embeddings.shape
    coarse_total = old_coarse.shape[0]
    fine_dev = old_fine.shape[0]
    sub_dev = pq_codes.shape[1]
    share = old_codebook.shape[0]
    code_total = share * blocks
    total = rows * blocks
    slot_max = max(4 * rows // blocks, 1)
    height = width + PACK + sub_dev
    block = pl.pallas_call(
        pack_kernel,
        out_shape=pltpu.VMEM((height, rows), jnp.bfloat16),
    )(embeddings, coarse_ids.reshape(1, rows), fine_ids.reshape(1, rows), pq_codes.T)
    parts = gather_blocks(block, blocks)
    vmem = pl.BlockSpec(memory_space=pltpu.VMEM)
    coarse_near, book_near = pl.pallas_call(
        stage_kernel,
        out_shape=(pltpu.VMEM(old_coarse.shape, jnp.float32), pltpu.VMEM(old_codebook.shape, jnp.float32)),
        in_specs=[vmem] * 2,
        cost_estimate=pl.CostEstimate(flops=10**6, bytes_accessed=10**6, transcendentals=0),
    )(old_coarse, old_codebook)
    hbm = pl.BlockSpec(memory_space=pltpu.HBM)
    new_coarse, new_fine, residual, new_book, error = pl.pallas_call(
        functools.partial(steps_kernel, blocks),
        out_shape=(
            jax.ShapeDtypeStruct(old_coarse.shape, jnp.float32),
            jax.ShapeDtypeStruct(old_fine.shape, jnp.float32),
            jax.ShapeDtypeStruct(embeddings.shape, jnp.bfloat16),
            jax.ShapeDtypeStruct(old_codebook.shape, jnp.float32),
            jax.ShapeDtypeStruct((1, rows), jnp.float32),
        ),
        in_specs=[vmem] * (blocks + 2) + [hbm],
        out_specs=(vmem, hbm, vmem, vmem, vmem),
        scratch_shapes=[
            pltpu.VMEM((fine_dev + GROUP, width), jnp.float32),
            pltpu.VMEM((height, total), jnp.bfloat16),
            pltpu.VMEM((width + PACK, total), jnp.bfloat16),
            pltpu.VMEM((total, 1, width), jnp.float32),
            pltpu.VMEM((width, total), jnp.bfloat16),
            pltpu.VMEM((width, code_total), jnp.float32),
            pltpu.VMEM((width, code_total), jnp.float32),
            pltpu.VMEM((total, sub_dev), jnp.float32),
            pltpu.VMEM((blocks * slot_max // GROUP, 128), jnp.int32),
            pltpu.SMEM((blocks * slot_max // GROUP, 128), jnp.int32),
        ]
        + [pltpu.SemaphoreType.DMA] * 3,
        compiler_params=pltpu.CompilerParams(vmem_limit_bytes=48 * 2**20),
    )(*parts, coarse_near, book_near, old_fine)
    row_error = jnp.sum(lax.all_gather(error, "rep", axis=0, tiled=True), axis=0) / (width * lax.axis_size("rep"))
    return (new_coarse, new_fine, residual, new_book, row_error)


def fits(sizes):
    rows, width, blocks, fine_dev, sub_dev, code_total, coarse_total, fine_total = sizes
    digits = 256
    return (
        blocks > 1
        and blocks & (blocks - 1) == 0
        and rows * blocks <= fine_dev
        and rows % 128 == 0
        and rows <= digits
        and coarse_total <= digits
        and code_total <= digits
        and fine_total <= digits * digits
        and width == code_total
        and width // sub_dev == PACK
        and sub_dev % PACK == 0
        and (4 * rows // blocks) % 128 == 0
    )


def shards(*args):
    embeddings, _, _, pq_codes, old_coarse, old_fine, old_codebook = args
    blocks = lax.axis_size("rows")
    rows, width = embeddings.shape
    fine_dev = old_fine.shape[0]
    sizes = (
        rows,
        width,
        blocks,
        fine_dev,
        pq_codes.shape[1],
        old_codebook.shape[0] * blocks,
        old_coarse.shape[0],
        fine_dev * blocks,
    )
    return gathered_shards(*args) if fits(sizes) else exchange_shards(*args)


def solution(mesh):
    placed = (
        P("rows", "rep"),
        P("rows"),
        P("rows"),
        P("rows", "rep"),
        P(None, "rep"),
        P("rows", "rep"),
        P("rows", "rep"),
    )
    return jax.shard_map(
        shards,
        mesh=mesh,
        in_specs=placed,
        out_specs=(P(None, "rep"), P("rows", "rep"), P("rows", "rep"), P("rows", "rep"), P("rows")),
        check_vma=False,
    )
```
